32 devices in a mesh: gx: 8 (over z, y), gy: 4 (over x, core).
Axes of the slice: x: 2, y: 2, z: 4, core: 2. Of those that a mesh axis runs over, the one named last changes fastest.
Arguments:
- right_side: float32 [128, 256, 512], P('gx', 'gy'), may hold values from -8 to 8
- guess: float32 [128, 256, 512], P('gx', 'gy'), may hold values from -4 to 4
- diagonal: float32 [128, 256, 512], P('gx', 'gy'), may hold values from 0.02 to 0.5
Outputs:
- solution_field: float32 [128, 256, 512], P('gx', 'gy')
- residual: float32 [128, 256, 512], P('gx', 'gy')
The draws below stay inside these ranges and needn't reach their ends.
All inputs are finite; a program needn't handle non-finite values.
Results may differ from the reference program's by a relative error of at most 0.00065.
Values sent between devices are 32-bit elements; how exact they have to be, the bound alone decides.
A program may use at most 128 MiB of HBM per device.

```python
import math
import jax
import jax.numpy as jnp
from jax import lax

NZ = 512
STEPS = 4
NX = 128
NY = 256


def level_of(rng, extent, cuts, smallest, largest):
    def one(position, parts):
        draws = jax.random.uniform(jax.random.fold_in(jax.random.fold_in(rng, 6), position), (parts,), jnp.float32, smallest / len(cuts), largest / len(cuts))
        return jnp.repeat(jnp.exp(draws), extent[position] // parts).reshape((-1,) + (1,) * (len(extent) - position - 1))

    gain = one(*cuts[0])
    for cut in cuts[1:]:
        gain = gain * one(*cut)
    return gain


def normal_values(own_key, dims, deviation, reach, cuts=(), held_as=jnp.bfloat16):
    drawn = jax.random.normal(own_key, dims, jnp.float32) * deviation
    if len(cuts) > 0:
        drawn = level_of(own_key, dims, cuts, -0.22, 0.18) * drawn
    return jnp.clip(drawn, min=-reach, max=reach).astype(held_as)


def setup_inputs(seed: int = 0) -> dict:
    splits = jax.random.split(jax.random.key(seed), 4)
    return {
        "right_side": normal_values(splits[0], (NX, NY, NZ), 1.0, 8.0, ((0, 8), (1, 4)), jnp.float32),
        "guess": normal_values(splits[1], (NX, NY, NZ), 0.5, 4.0, ((0, 8), (1, 4)), jnp.float32),
        "diagonal": jnp.clip(jnp.exp(math.log(0.5) - 3.218876 * jax.random.uniform(splits[2], (NX, NY, NZ), jnp.float32) ** level_of(splits[2], (NX, NY, NZ), ((0, 8), (1, 4)), -0.2, 0.2)), 0.02, 0.5),
    }


center_shift = 6.25
half_range = 6.25


def operate(field, diagonal):
    padded = jnp.pad(field, 1)
    beside = padded[2:, 1:-1, 1:-1] + padded[:-2, 1:-1, 1:-1]
    beside = beside + padded[1:-1, 2:, 1:-1] + padded[1:-1, :-2, 1:-1]
    beside = beside + padded[1:-1, 1:-1, 2:] + padded[1:-1, 1:-1, :-2]
    return (6.0 + diagonal) * field - beside


def change_matrix(depth):
    rows = []
    for i in range(depth + 1):
        line = []
        for k in range(depth + 1):
            value = 0.0
            if k == 0:
                value = center_shift if i == 0 else (half_range if i == 1 else 0.0)
            elif k < depth:
                if i == k:
                    value = center_shift
                elif i == k - 1 or i == k + 1:
                    value = half_range / 2.0
            line.append(value)
        rows.append(line)
    return jnp.array(rows, dtype=jnp.float32)


def quad(left, matrix, right):
    return jnp.sum(left * jnp.dot(matrix, right, precision=lax.Precision.HIGHEST))


def coefficient_steps(gram, depth):
    change = change_matrix(depth)
    unit = jnp.zeros((depth + 1,), jnp.float32).at[0].set(1.0)
    xc = jnp.zeros((depth + 1,), jnp.float32)
    rc = unit
    pc = unit
    for step in range(depth):
        rr = quad(rc, gram, rc)
        moved = jnp.dot(change, pc, precision=lax.Precision.HIGHEST)
        alpha = rr / quad(pc, gram, moved)
        xc = xc + alpha * pc
        rc = rc - alpha * moved
        beta = quad(rc, gram, rc) / rr
        pc = rc + beta * pc
    return xc, rc


def reference(right_side, guess, diagonal):
    first = right_side - operate(guess, diagonal)
    basis = [first]
    for k in range(STEPS):
        applied = operate(basis[k], diagonal)
        if k == 0:
            nextone = (applied - center_shift * basis[k]) / half_range
        else:
            nextone = 2.0 * (applied - center_shift * basis[k]) / half_range - basis[k - 1]
        basis.append(nextone)
    stacked = jnp.stack(basis).reshape(STEPS + 1, -1)
    gram = jnp.dot(stacked, stacked.T, precision=lax.Precision.HIGHEST)
    xc, rc = coefficient_steps(gram, STEPS)
    solution_field = guess
    residual = jnp.zeros_like(guess)
    for k in range(STEPS + 1):
        solution_field = solution_field + xc[k] * basis[k]
        residual = residual + rc[k] * basis[k]
    return solution_field, residual
```

```python
import functools
import jax
import jax.numpy as jnp
from jax import lax
from jax.experimental import pallas as pl
from jax.experimental.pallas import tpu as pltpu
from jax.sharding import PartitionSpec as P

STEPS = 4
center_shift = 6.25
half_range = 6.25
PAD = 8
MESH = pl.DeviceIdType.MESH


def change_matrix(depth):
    rows = []
    for i in range(depth + 1):
        line = []
        for k in range(depth + 1):
            value = 0.0
            if k == 0:
                value = center_shift if i == 0 else half_range if i == 1 else 0.0
            elif k < depth:
                if i == k:
                    value = center_shift
                elif i == k - 1 or i == k + 1:
                    value = half_range / 2.0
            line.append(value)
        rows.append(line)
    return rows


def total(terms):
    terms = list(terms)
    while len(terms) > 1:
        pairs = [a + b for a, b in zip(terms[::2], terms[1::2])]
        terms = pairs + ([terms[-1]] if len(terms) % 2 else [])
    return terms[0]


def quad(left, gram, right):
    return total(l * total(g * r for g, r in zip(line, right)) for l, line in zip(left, gram))


def moved_by(change, pc):
    lines = [[c * p for c, p in zip(line, pc) if c != 0.0] for line in change]
    return [total(terms) for terms in lines]


def coefficient_steps(gram, depth, zero, one):
    change = [line[:depth] for line in change_matrix(depth)]
    unit = [one] + [zero] * (depth - 1)
    xc, rc, pc = [zero] * depth, unit, unit
    rr = quad(rc, gram, rc)
    for step in range(depth - 1):
        moved = moved_by(change[:depth], pc)
        alpha = rr / quad(pc, gram, moved)
        xc = [x + alpha * p for x, p in zip(xc, pc)]
        rc = [r - alpha * m for r, m in zip(rc, moved)]
        new = quad(rc, gram, rc)
        beta = new / rr
        pc = [r + beta * p for r, p in zip(rc, pc)]
        rr = new
    moved = moved_by(change, pc)
    return xc + [zero], rc + [zero], pc + [zero], moved, rr


def gram_of(moments, size):
    return [
        [0.5 * (moments[i + j] + moments[abs(i - j)]) for j in range(size)] for i in range(size)
    ]


def reach(count, known):
    steps = []
    while known < count - 1:
        steps.append(max(known, 1))
        known += steps[-1]
    return steps


def fold(p):
    rows, cols = p.shape
    return total(
        p[i : i + 8, j : j + 128] for i in range(0, rows, 8) for j in range(0, cols, 128)
    )


def kernel(px, py, rows, r_hbm, g_hbm, d_hbm, sol_out, step_out, res_out, moved_out, alpha_out,
           F, R, D, Ys, Yr, A, M, acc,
           edge_sem, load_sem, xs_sem, xr_sem, ys_sem, yr_sem, as_sem, ar_sem, met_sem):
    ZC, LX, LY, _ = R.shape
    NC = LY // rows
    gx, gy = lax.axis_index("gx"), lax.axis_index("gy")
    low_x, high_x, low_y, high_y = gx > 0, gx < px - 1, gy > 0, gy < py - 1
    inner = pl.ds(PAD, LY)

    def column(z):
        return pl.ds(z * 128, 128)

    edges, loads = [], []
    for z in range(ZC):
        for i, x in enumerate((0, LX - 1)):
            edges.append(pltpu.make_async_copy(
                g_hbm.at[x, :, column(z)], F.at[0, z, x + 1, inner, :], edge_sem.at[z, i]))
    for z in range(ZC):
        loads.append(pltpu.make_async_copy(
            g_hbm.at[pl.ds(1, LX - 2), :, column(z)],
            F.at[0, z, pl.ds(2, LX - 2), inner, :], load_sem.at[0, z]))
    for i, (src, dst) in enumerate(((d_hbm, D), (r_hbm, R))):
        for z in range(ZC):
            loads.append(pltpu.make_async_copy(
                src.at[:, :, column(z)], dst.at[z], load_sem.at[1 + i, z]))
    for copy in edges + loads:
        copy.start()

    x_has, y_has = (low_x, high_x), (low_y, high_y)

    def partners(axis, distance):
        me, count = (gx, px) if axis == "gx" else (gy, py)
        return [(me >= distance, {axis: me - distance}), (me < count - distance, {axis: me + distance})]

    def greet(sem, pairs):
        for there, device in pairs:
            pl.when(there)(lambda: pl.semaphore_signal(sem, inc=1, device_id=device, device_id_type=MESH))

    def meet(sem, pairs):
        pl.semaphore_wait(sem, sum(there.astype(jnp.int32) for there, _ in pairs))

    barrier = pltpu.get_barrier_semaphore()
    beside = partners("gx", 1) + partners("gy", 1)
    greet(barrier, beside)

    def zero_planes(x):
        def one(j, carry):
            at = pl.multiple_of(PAD + j * 8, 8)
            for k in range(STEPS + 1):
                for z in range(ZC):
                    F[k, z, x, pl.ds(at, 8), :] = jnp.zeros((8, 128), jnp.float32)
            return carry
        lax.fori_loop(0, LY // 8, one, 0)

    pl.when(jnp.logical_not(low_x))(lambda: zero_planes(0))
    pl.when(jnp.logical_not(high_x))(lambda: zero_planes(LX + 1))

    def zero_rows(side):
        for k in range(STEPS + 1):
            Yr[k, side] = jnp.zeros((ZC, LX, 128), jnp.float32)

    pl.when(jnp.logical_not(low_y))(lambda: zero_rows(0))
    pl.when(jnp.logical_not(high_y))(lambda: zero_rows(1))

    meet(barrier, beside)

    meetings = [("gx", o) for o in reach(px, 1)] + [("gy", o) for o in reach(py, 0)]
    met = []

    def spread(last=False):
        while len(met) <= len(meetings):
            n = len(met)
            if n > 0:
                meet(met_sem.at[n - 1], partners(*meetings[n - 1]))
            if n < len(meetings):
                greet(met_sem.at[n], partners(*meetings[n]))
            met.append(n)
            if not last:
                break

    me = gx * py + gy

    def send_sums(stage, row):
        A[stage] = row
        M[stage, me] = row
        for ox in range(px):
            for oy in range(py):
                if ox or oy:
                    pltpu.make_async_remote_copy(
                        src_ref=A.at[stage], dst_ref=M.at[stage, me],
                        send_sem=as_sem.at[stage], recv_sem=ar_sem.at[stage],
                        device_id={"gx": lax.rem(gx + ox, px), "gy": lax.rem(gy + oy, py)},
                        device_id_type=MESH,
                    ).start()

    def all_sums(stage):
        peers = pl.ds(0, px * py - 1)
        return pltpu.make_async_remote_copy(
            src_ref=M.at[stage, peers], dst_ref=M.at[stage, peers],
            send_sem=as_sem.at[stage], recv_sem=ar_sem.at[stage],
            device_id={"gx": lax.rem(gx + 1, px)}, device_id_type=MESH,
        )

    def x_copy(k, side, j):
        at = pl.ds(PAD + j * rows, rows)
        return pltpu.make_async_remote_copy(
            src_ref=F.at[k, :, 1 if side == 0 else LX, at, :],
            dst_ref=F.at[k, :, LX + 1 if side == 0 else 0, at, :],
            send_sem=xs_sem.at[k, side, j],
            recv_sem=xr_sem.at[k, side, j],
            device_id={"gx": gx - 1 if side == 0 else gx + 1},
            device_id_type=MESH,
        )

    def y_copy(k, side):
        return pltpu.make_async_remote_copy(
            src_ref=Ys.at[k, side],
            dst_ref=Yr.at[k, 1 - side],
            send_sem=ys_sem.at[k, side],
            recv_sem=yr_sem.at[k, side],
            device_id={"gy": gy - 1 if side == 0 else gy + 1},
            device_id_type=MESH,
        )

    def send_x(k, j):
        for side in (0, 1):
            pl.when(x_has[side])(lambda: x_copy(k, side, j).start())

    def wait_x(k, j):
        for side in (0, 1):
            pl.when(x_has[1 - side])(lambda: x_copy(k, side, j).wait_recv())

    def send_y(k):
        for x in range(LX):
            for z in range(ZC):
                Ys[k, 0, z, x : x + 1, :] = F[k, z, x + 1, PAD : PAD + 1, :]
                Ys[k, 1, z, x : x + 1, :] = F[k, z, x + 1, PAD + LY - 1 : PAD + LY, :]
        for side in (0, 1):
            pl.when(y_has[side])(lambda: y_copy(k, side).start())

    def wait_y(k):
        for side in (0, 1):
            pl.when(y_has[1 - side])(lambda: y_copy(k, side).wait_recv())
        for x in range(LX):
            for z in range(ZC):
                F[k, z, x + 1, PAD - 1 : PAD, :] = Yr[k, 0, z, x : x + 1, :]
                F[k, z, x + 1, PAD + LY : PAD + LY + 1, :] = Yr[k, 1, z, x : x + 1, :]

    order = [0] + ([NC - 1] if NC > 1 else []) + list(range(1, NC - 1))
    for copy in edges:
        copy.wait()
    for j in order:
        send_x(0, j)

    acc[...] = jnp.zeros(acc.shape, jnp.float32)
    zero_tile = jnp.zeros((8, 128), jnp.float32)

    c_scale = 2.0 / half_range

    def block(k, x, y, n):
        at, up, down = pl.ds(PAD + y, n), pl.ds(PAD + y + 1, n), pl.ds(PAD + y - 1, n)
        lane = lax.broadcasted_iota(jnp.int32, (n, 128), 1)
        first_lane, last_lane = lane == 0, lane == 127
        here = [F[k - 1, z, x, at, :] for z in range(ZC)]
        right = [pltpu.roll(h, 1, 1) for h in here]
        left = [pltpu.roll(h, 127, 1) for h in here]
        squares, crosses = [], []
        for z in range(ZC):
            beside = F[k - 1, z, x + 1, at, :] + F[k - 1, z, x - 1, at, :]
            beside = beside + (F[k - 1, z, x, up, :] + F[k - 1, z, x, down, :])
            before = jnp.where(first_lane, right[z - 1] if z > 0 else 0.0, right[z])
            after = jnp.where(last_lane, left[z + 1] if z < ZC - 1 else 0.0, left[z])
            beside = beside + (before + after)
            diag = D[z, x - 1, pl.ds(y, n), :]
            if k == 1:
                new = R[z, x - 1, pl.ds(y, n), :] - ((6.0 + diag) * here[z] - beside)
                D[z, x - 1, pl.ds(y, n), :] = (diag + (6.0 - center_shift)) * c_scale
            elif k == 2:
                new = (diag * here[z] - beside * c_scale) * 0.5
            else:
                new = diag * here[z] - beside * c_scale - F[k - 2, z, x, at, :]
            F[k, z, x, at, :] = new
            squares.append(fold(new * new))
            if k > 1:
                crosses.append(fold(new * here[z]))
        return total(squares), (total(crosses) if k > 1 else zero_tile)

    def add(a, b):
        return a[0] + b[0], a[1] + b[1]

    for copy in loads[:ZC]:
        copy.wait()
    send_y(0)
    for copy in loads[ZC:]:
        copy.wait()

    lane = lax.broadcasted_iota(jnp.int32, (1, 128), 1)

    def row_of(sums):
        row = jnp.zeros((1, 128), jnp.float32)
        for m, part in sums:
            s = jnp.sum(jnp.sum(part, axis=0, keepdims=True), axis=1, keepdims=True)
            row = row + jnp.where(lane == m, s, 0.0)
        return row

    def moments_of(stage, which):
        all_sums(stage).wait_recv()
        row = total(M[stage, i] for i in range(px * py))
        return {
            m: jnp.broadcast_to(jnp.sum(jnp.where(lane == m, row, 0.0), axis=1, keepdims=True), (8, 128))
            for m in which
        }

    for k in range(1, STEPS + 1):
        sums = (zero_tile, zero_tile)
        wait_y(k - 1)
        for i, j in enumerate(order):
            wait_x(k - 1, j)
            for x in (1, LX):
                sums = add(sums, block(k, x, j * rows, rows))
            send_x(k, j)
            if i == 1:
                send_y(k)
            if i == 0:
                spans = [(0, 8), (LY - 8, 8)]
            elif i < NC - 1:
                spans = [(8 + (i - 1) * rows, rows)]
            else:
                spans = [(8 + (i - 1) * rows, LY - 16 - (i - 1) * rows)]

            def plane(x, s):
                for y, n in spans:
                    s = add(s, block(k, x, y, n))
                return s

            sums = lax.fori_loop(2, LX, plane, sums, unroll=7 if (LX - 2) % 7 == 0 else 2)
            if i % 2 == 0:
                spread()
        acc[2 * (k - 1)] = sums[0]
        if k > 1:
            acc[2 * (k - 1) - 1] = sums[1]

    spread(last=True)
    early, late = range(2 * STEPS - 1), range(2 * STEPS - 1, 2 * STEPS + 1)
    send_sums(0, row_of([(m, acc[m]) for m in early]))

    last = STEPS + 1
    wait_y(last - 1)

    def inner_plane(x, s):
        for y in range(0, LY, rows):
            s = add(s, block(last, x, y, rows))
        return s

    sums = lax.fori_loop(2, LX, inner_plane, (zero_tile, zero_tile))
    for j in order:
        wait_x(last - 1, j)
        for x in (1, LX):
            sums = add(sums, block(last, x, j * rows, rows))
    send_sums(1, row_of([(2 * STEPS - 1, sums[1]), (2 * STEPS, sums[0])]))

    got = moments_of(0, early)

    def moment(m):
        return got[m] if m < 2 else 2.0 * got[m] - got[m % 2]

    moments = [moment(m) for m in early]
    zero, one = jnp.zeros((8, 128), jnp.float32), jnp.ones((8, 128), jnp.float32)
    xc, rc, pc, moved, rr = coefficient_steps(gram_of(moments, STEPS), STEPS, zero, one)

    def plane(x, carry):
        for i in range(LY // 8):
            at, to = pl.ds(PAD + i * 8, 8), pl.ds(i * 8, 8)
            for z in range(ZC):
                basis = [F[k + 1, z, x + 1, at, :] for k in range(STEPS + 1)]
                sol = F[0, z, x + 1, at, :]
                for k in range(STEPS + 1):
                    sol = sol + xc[k] * basis[k]
                sol_out[x, to, column(z)] = sol
                for out, coefficients in ((step_out, pc), (res_out, rc), (moved_out, moved)):
                    out[x, to, column(z)] = total(c * b for c, b in zip(coefficients, basis))
        return carry

    lax.fori_loop(0, LX, plane, 0)

    got.update(moments_of(1, late))
    moments += [moment(m) for m in late]
    alpha_out[...] = rr / quad(pc, gram_of(moments, STEPS + 1), moved)

    for k in range(STEPS + 1):
        for side in (0, 1):
            def done():
                for j in range(NC):
                    x_copy(k, side, j).wait_send()
            pl.when(x_has[side])(done)
            pl.when(y_has[side])(lambda: y_copy(k, side).wait_send())
    for stage in (0, 1):
        all_sums(stage).wait_send()


def last_step(sol_ref, step_ref, res_ref, moved_ref, alpha_ref, sol_hbm, res_hbm, sol, res, sems):
    LX, LY, LZ = sol.shape
    alpha = jnp.concatenate([alpha_ref[...]] * (LZ // 128), axis=1)
    n = 2 if LX % 2 == 0 else 1
    copies = []
    for x in range(0, LX, n):
        for i, (out, hbm) in enumerate(((sol, sol_hbm), (res, res_hbm))):
            for p in range(x, x + n):
                for y in range(0, LY, 8):
                    at = (p, pl.ds(y, 8), slice(None))
                    if i == 0:
                        out[at] = sol_ref[at] + alpha * step_ref[at]
                    else:
                        out[at] = res_ref[at] - alpha * moved_ref[at]
            planes = pl.ds(x, n)
            copies.append(pltpu.make_async_copy(out.at[planes], hbm.at[planes], sems.at[i, x // n]))
            copies[-1].start()
    for copy in copies:
        copy.wait()


def solution(mesh):
    px, py = mesh.shape["gx"], mesh.shape["gy"]

    def shards(right_side, guess, diagonal):
        LX, LY, LZ = guess.shape
        rows = 16
        NC, ZC = LY // rows, LZ // 128
        n = STEPS + 1
        dma = pltpu.SemaphoreType.DMA
        like = jax.ShapeDtypeStruct(guess.shape, jnp.float32)
        vmem, hbm = pl.BlockSpec(memory_space=pltpu.VMEM), pl.BlockSpec(memory_space=pltpu.MemorySpace.HBM)
        parts = pl.pallas_call(
            functools.partial(kernel, px, py, rows),
            out_shape=(like,) * 4 + (jax.ShapeDtypeStruct((8, 128), jnp.float32),),
            in_specs=[hbm] * 3,
            out_specs=(vmem,) * 5,
            scratch_shapes=[
                pltpu.VMEM((n + 1, ZC, LX + 2, LY + 3 * PAD, 128), jnp.float32),
                pltpu.VMEM((ZC, LX, LY, 128), jnp.float32),
                pltpu.VMEM((ZC, LX, LY, 128), jnp.float32),
                pltpu.VMEM((n, 2, ZC, LX, 128), jnp.float32),
                pltpu.VMEM((n, 2, ZC, LX, 128), jnp.float32),
                pltpu.VMEM((2, 1, 128), jnp.float32),
                pltpu.VMEM((2, px * py, 1, 128), jnp.float32),
                pltpu.VMEM((2 * STEPS + 1, 8, 128), jnp.float32),
                dma((ZC, 2)), dma((3, ZC)), dma((n, 2, NC)), dma((n, 2, NC)), dma((n, 2)), dma((n, 2)),
                dma((2,)), dma((2,)),
                pltpu.SemaphoreType.REGULAR((len(reach(px, 1)) + len(reach(py, 0)),)),
            ],
            compiler_params=pltpu.CompilerParams(
                collective_id=0, has_side_effects=True, vmem_limit_bytes=44 * 1024 * 1024
            ),
        )(right_side, guess, diagonal)
        return pl.pallas_call(
            last_step,
            out_shape=(like,) * 2,
            in_specs=[vmem] * 5,
            out_specs=(hbm,) * 2,
            scratch_shapes=[pltpu.VMEM(guess.shape, jnp.float32)] * 2 + [dma((2, LX))],
            compiler_params=pltpu.CompilerParams(vmem_limit_bytes=40 * 1024 * 1024),
        )(*parts)

    spec = P("gx", "gy", None)
    return jax.shard_map(
        shards, mesh=mesh, in_specs=(spec,) * 3, out_specs=(spec,) * 2, check_vma=False
    )
```

```python
import functools
import jax
import jax.numpy as jnp
from jax import lax
from jax.experimental import pallas as pl
from jax.experimental.pallas import tpu as pltpu
from jax.sharding import PartitionSpec as P

STEPS = 4
center_shift = 6.25
half_range = 6.25
PAD = 8
MESH = pl.DeviceIdType.MESH


def change_matrix(depth):
    rows = []
    for i in range(depth + 1):
        line = []
        for k in range(depth + 1):
            value = 0.0
            if k == 0:
                value = center_shift if i == 0 else half_range if i == 1 else 0.0
            elif k < depth:
                if i == k:
                    value = center_shift
                elif i == k - 1 or i == k + 1:
                    value = half_range / 2.0
            line.append(value)
        rows.append(line)
    return rows


def total(terms):
    terms = list(terms)
    while len(terms) > 1:
        pairs = [a + b for a, b in zip(terms[::2], terms[1::2])]
        terms = pairs + ([terms[-1]] if len(terms) % 2 else [])
    return terms[0]


def quad(left, gram, right):
    return total(l * total(g * r for g, r in zip(line, right)) for l, line in zip(left, gram))


def moved_by(change, pc):
    lines = [[c * p for c, p in zip(line, pc) if c != 0.0] for line in change]
    return [total(terms) for terms in lines]


def coefficient_steps(gram, depth, zero, one):
    change = [line[:depth] for line in change_matrix(depth)]
    unit = [one] + [zero] * (depth - 1)
    xc, rc, pc = [zero] * depth, unit, unit
    rr = quad(rc, gram, rc)
    for step in range(depth - 1):
        moved = moved_by(change[:depth], pc)
        alpha = rr / quad(pc, gram, moved)
        xc = [x + alpha * p for x, p in zip(xc, pc)]
        rc = [r - alpha * m for r, m in zip(rc, moved)]
        new = quad(rc, gram, rc)
        beta = new / rr
        pc = [r + beta * p for r, p in zip(rc, pc)]
        rr = new
    moved = moved_by(change, pc)
    return xc + [zero], rc + [zero], pc + [zero], moved, rr


def gram_of(moments, size):
    return [
        [0.5 * (moments[i + j] + moments[abs(i - j)]) for j in range(size)] for i in range(size)
    ]


def reach(count, known):
    steps = []
    while known < count - 1:
        steps.append(max(known, 1))
        known += steps[-1]
    return steps


def fold(p):
    rows, cols = p.shape
    return total(
        p[i : i + 8, j : j + 128] for i in range(0, rows, 8) for j in range(0, cols, 128)
    )


def kernel(px, py, rows, r_hbm, g_hbm, d_hbm, sol_out, step_out, res_out, moved_out, alpha_out,
           F, R, D, Ys, Yr, A, M, acc,
           edge_sem, load_sem, xs_sem, xr_sem, ys_sem, yr_sem, as_sem, ar_sem, met_sem):
    ZC, LX, LY, _ = R.shape
    NC = LY // rows
    gx, gy = lax.axis_index("gx"), lax.axis_index("gy")
    low_x, high_x, low_y, high_y = gx > 0, gx < px - 1, gy > 0, gy < py - 1
    inner = pl.ds(PAD, LY)

    def column(z):
        return pl.ds(z * 128, 128)

    edges, loads = [], []
    for z in range(ZC):
        for i, x in enumerate((0, LX - 1)):
            edges.append(pltpu.make_async_copy(
                g_hbm.at[x, :, column(z)], F.at[0, z, x + 1, inner, :], edge_sem.at[z, i]))
    for z in range(ZC):
        loads.append(pltpu.make_async_copy(
            g_hbm.at[pl.ds(1, LX - 2), :, column(z)],
            F.at[0, z, pl.ds(2, LX - 2), inner, :], load_sem.at[0, z]))
    for i, (src, dst) in enumerate(((d_hbm, D), (r_hbm, R))):
        for z in range(ZC):
            loads.append(pltpu.make_async_copy(
                src.at[:, :, column(z)], dst.at[z], load_sem.at[1 + i, z]))
    for copy in edges + loads:
        copy.start()

    x_has, y_has = (low_x, high_x), (low_y, high_y)

    def partners(axis, distance):
        me, count = (gx, px) if axis == "gx" else (gy, py)
        return [(me >= distance, {axis: me - distance}), (me < count - distance, {axis: me + distance})]

    def greet(sem, pairs):
        for there, device in pairs:
            pl.when(there)(lambda: pl.semaphore_signal(sem, inc=1, device_id=device, device_id_type=MESH))

    def meet(sem, pairs):
        pl.semaphore_wait(sem, sum(there.astype(jnp.int32) for there, _ in pairs))

    barrier = pltpu.get_barrier_semaphore()
    beside = partners("gx", 1) + partners("gy", 1)
    greet(barrier, beside)

    def zero_planes(x):
        def one(j, carry):
            at = pl.multiple_of(PAD + j * 8, 8)
            for k in range(STEPS + 1):
                for z in range(ZC):
                    F[k, z, x, pl.ds(at, 8), :] = jnp.zeros((8, 128), jnp.float32)
            return carry
        lax.fori_loop(0, LY // 8, one, 0)

    pl.when(jnp.logical_not(low_x))(lambda: zero_planes(0))
    pl.when(jnp.logical_not(high_x))(lambda: zero_planes(LX + 1))

    def zero_rows(side):
        for k in range(STEPS + 1):
            Yr[k, side] = jnp.zeros((ZC, LX, 128), jnp.float32)

    pl.when(jnp.logical_not(low_y))(lambda: zero_rows(0))
    pl.when(jnp.logical_not(high_y))(lambda: zero_rows(1))

    meet(barrier, beside)

    meetings = [("gx", o) for o in reach(px, 1)] + [("gy", o) for o in reach(py, 0)]
    met = []

    def spread(last=False):
        while len(met) <= len(meetings):
            n = len(met)
            if n > 0:
                meet(met_sem.at[n - 1], partners(*meetings[n - 1]))
            if n < len(meetings):
                greet(met_sem.at[n], partners(*meetings[n]))
            met.append(n)
            if not last:
                break

    me = gx * py + gy

    def send_sums(stage, row):
        A[stage] = row
        M[stage, me] = row
        for ox in range(px):
            to_x = jnp.where(gx < px // 2, px - 1 - ox, ox)
            for oy in range(py):
                to_y = jnp.where(gy < py // 2, py - 1 - oy, oy)

                @pl.when(jnp.logical_or(to_x != gx, to_y != gy))
                def _():
                    pltpu.make_async_remote_copy(
                        src_ref=A.at[stage], dst_ref=M.at[stage, me],
                        send_sem=as_sem.at[stage], recv_sem=ar_sem.at[stage],
                        device_id={"gx": to_x, "gy": to_y}, device_id_type=MESH,
                    ).start()

    def all_sums(stage):
        peers = pl.ds(0, px * py - 1)
        return pltpu.make_async_remote_copy(
            src_ref=M.at[stage, peers], dst_ref=M.at[stage, peers],
            send_sem=as_sem.at[stage], recv_sem=ar_sem.at[stage],
            device_id={"gx": lax.rem(gx + 1, px)}, device_id_type=MESH,
        )

    def x_copy(k, side, j):
        at = pl.ds(PAD + j * rows, rows)
        return pltpu.make_async_remote_copy(
            src_ref=F.at[k, :, 1 if side == 0 else LX, at, :],
            dst_ref=F.at[k, :, LX + 1 if side == 0 else 0, at, :],
            send_sem=xs_sem.at[k, side, j],
            recv_sem=xr_sem.at[k, side, j],
            device_id={"gx": gx - 1 if side == 0 else gx + 1},
            device_id_type=MESH,
        )

    def y_copy(k, side):
        return pltpu.make_async_remote_copy(
            src_ref=Ys.at[k, side],
            dst_ref=Yr.at[k, 1 - side],
            send_sem=ys_sem.at[k, side],
            recv_sem=yr_sem.at[k, side],
            device_id={"gy": gy - 1 if side == 0 else gy + 1},
            device_id_type=MESH,
        )

    def send_x(k, j):
        for side in (0, 1):
            pl.when(x_has[side])(lambda: x_copy(k, side, j).start())

    def wait_x(k, j):
        for side in (0, 1):
            pl.when(x_has[1 - side])(lambda: x_copy(k, side, j).wait_recv())

    def send_y(k):
        for x in range(LX):
            for z in range(ZC):
                Ys[k, 0, z, x : x + 1, :] = F[k, z, x + 1, PAD : PAD + 1, :]
                Ys[k, 1, z, x : x + 1, :] = F[k, z, x + 1, PAD + LY - 1 : PAD + LY, :]
        for side in (0, 1):
            pl.when(y_has[side])(lambda: y_copy(k, side).start())

    def wait_y(k):
        for side in (0, 1):
            pl.when(y_has[1 - side])(lambda: y_copy(k, side).wait_recv())
        for x in range(LX):
            for z in range(ZC):
                F[k, z, x + 1, PAD - 1 : PAD, :] = Yr[k, 0, z, x : x + 1, :]
                F[k, z, x + 1, PAD + LY : PAD + LY + 1, :] = Yr[k, 1, z, x : x + 1, :]

    order = [0] + ([NC - 1] if NC > 1 else []) + list(range(1, NC - 1))
    for copy in edges:
        copy.wait()
    for j in order:
        send_x(0, j)

    acc[...] = jnp.zeros(acc.shape, jnp.float32)
    zero_tile = jnp.zeros((8, 128), jnp.float32)

    c_scale = 2.0 / half_range

    def block(k, x, y, n, without=None):
        at, up, down = pl.ds(PAD + y, n), pl.ds(PAD + y + 1, n), pl.ds(PAD + y - 1, n)
        lane = lax.broadcasted_iota(jnp.int32, (n, 128), 1)
        first_lane, last_lane = lane == 0, lane == 127
        here = [F[k - 1, z, x, at, :] for z in range(ZC)]
        right = [pltpu.roll(h, 1, 1) for h in here]
        left = [pltpu.roll(h, 127, 1) for h in here]
        squares, crosses = [], []
        for z in range(ZC):
            inside = [p for p in (x + 1, x - 1) if without is None or p != without]
            beside = total(F[k - 1, z, p, at, :] for p in inside)
            beside = beside + (F[k - 1, z, x, up, :] + F[k - 1, z, x, down, :])
            before = jnp.where(first_lane, right[z - 1] if z > 0 else 0.0, right[z])
            after = jnp.where(last_lane, left[z + 1] if z < ZC - 1 else 0.0, left[z])
            beside = beside + (before + after)
            diag = D[z, x - 1, pl.ds(y, n), :]
            if k == 1:
                new = R[z, x - 1, pl.ds(y, n), :] - ((6.0 + diag) * here[z] - beside)
                D[z, x - 1, pl.ds(y, n), :] = (diag + (6.0 - center_shift)) * c_scale
            elif k == 2:
                new = (diag * here[z] - beside * c_scale) * 0.5
            else:
                new = diag * here[z] - beside * c_scale - F[k - 2, z, x, at, :]
            F[k, z, x, at, :] = new
            if without is not None:
                continue
            squares.append(fold(new * new))
            if k > 1:
                crosses.append(fold(new * here[z]))
        if without is None:
            return total(squares), (total(crosses) if k > 1 else zero_tile)

    def complete(k, x, beyond, y, n):
        at = pl.ds(PAD + y, n)
        squares, crosses = [], []
        for z in range(ZC):
            new = F[k, z, x, at, :] - c_scale * F[k - 1, z, beyond, at, :]
            F[k, z, x, at, :] = new
            squares.append(fold(new * new))
            crosses.append(fold(new * F[k - 1, z, x, at, :]))
        return total(squares), total(crosses)

    def add(a, b):
        return a[0] + b[0], a[1] + b[1]

    for copy in loads[:ZC]:
        copy.wait()
    send_y(0)
    for copy in loads[ZC:]:
        copy.wait()

    lane = lax.broadcasted_iota(jnp.int32, (1, 128), 1)

    def row_of(sums):
        row = jnp.zeros((1, 128), jnp.float32)
        for m, part in sums:
            s = jnp.sum(jnp.sum(part, axis=0, keepdims=True), axis=1, keepdims=True)
            row = row + jnp.where(lane == m, s, 0.0)
        return row

    def moments_of(stage, which):
        all_sums(stage).wait_recv()
        row = total(M[stage, i] for i in range(px * py))
        return {
            m: jnp.broadcast_to(jnp.sum(jnp.where(lane == m, row, 0.0), axis=1, keepdims=True), (8, 128))
            for m in which
        }

    for k in range(1, STEPS + 1):
        sums = (zero_tile, zero_tile)
        wait_y(k - 1)
        for i, j in enumerate(order):
            wait_x(k - 1, j)
            for x in (1, LX):
                sums = add(sums, block(k, x, j * rows, rows))
            send_x(k, j)
            if i == 1:
                send_y(k)
            if i == 0:
                spans = [(0, 8), (LY - 8, 8)]
            elif i < NC - 1:
                spans = [(8 + (i - 1) * rows, rows)]
            else:
                spans = [(8 + (i - 1) * rows, LY - 16 - (i - 1) * rows)]

            def plane(x, s):
                for y, n in spans:
                    s = add(s, block(k, x, y, n))
                return s

            sums = lax.fori_loop(2, LX, plane, sums, unroll=7 if (LX - 2) % 7 == 0 else 2)
            if i % 2 == 0:
                spread()
        acc[2 * (k - 1)] = sums[0]
        if k > 1:
            acc[2 * (k - 1) - 1] = sums[1]

    spread(last=True)
    early, late = range(2 * STEPS - 1), range(2 * STEPS - 1, 2 * STEPS + 1)
    send_sums(0, row_of([(m, acc[m]) for m in early]))

    last = STEPS + 1
    wait_y(last - 1)

    def inner_plane(x, s):
        for y in range(0, LY, rows):
            s = add(s, block(last, x, y, rows))
        return s

    sums = lax.fori_loop(2, LX, inner_plane, (zero_tile, zero_tile))
    ends = ((1, 0), (LX, LX + 1))
    for x, beyond in ends:
        for j in order:
            block(last, x, j * rows, rows, without=beyond)
    for j in order:
        wait_x(last - 1, j)
        for x, beyond in ends:
            sums = add(sums, complete(last, x, beyond, j * rows, rows))
    send_sums(1, row_of([(2 * STEPS - 1, sums[1]), (2 * STEPS, sums[0])]))

    got = moments_of(0, early)

    def moment(m):
        return got[m] if m < 2 else 2.0 * got[m] - got[m % 2]

    moments = [moment(m) for m in early]
    zero, one = jnp.zeros((8, 128), jnp.float32), jnp.ones((8, 128), jnp.float32)
    xc, rc, pc, moved, rr = coefficient_steps(gram_of(moments, STEPS), STEPS, zero, one)

    def plane(x, carry):
        for i in range(LY // 8):
            at, to = pl.ds(PAD + i * 8, 8), pl.ds(i * 8, 8)
            for z in range(ZC):
                basis = [F[k + 1, z, x + 1, at, :] for k in range(STEPS + 1)]
                sol = F[0, z, x + 1, at, :]
                for k in range(STEPS + 1):
                    sol = sol + xc[k] * basis[k]
                sol_out[x, to, column(z)] = sol
                for out, coefficients in ((step_out, pc), (res_out, rc), (moved_out, moved)):
                    out[x, to, column(z)] = total(c * b for c, b in zip(coefficients, basis))
        return carry

    lax.fori_loop(0, LX, plane, 0)

    for k in range(STEPS + 1):
        for side in (0, 1):
            def done():
                for j in range(NC):
                    x_copy(k, side, j).wait_send()
            pl.when(x_has[side])(done)
            pl.when(y_has[side])(lambda: y_copy(k, side).wait_send())
    all_sums(0).wait_send()

    got.update(moments_of(1, late))
    moments += [moment(m) for m in late]
    alpha_out[...] = rr / quad(pc, gram_of(moments, STEPS + 1), moved)

    all_sums(1).wait_send()


def last_step(sol_ref, step_ref, res_ref, moved_ref, alpha_ref, sol_hbm, res_hbm, sol, res, sems):
    LX, LY, LZ = sol.shape
    alpha = jnp.concatenate([alpha_ref[...]] * (LZ // 128), axis=1)
    n = 1
    copies = []
    for x in range(0, LX, n):
        for i, (out, hbm) in enumerate(((sol, sol_hbm), (res, res_hbm))):
            for p in range(x, x + n):
                for y in range(0, LY, 8):
                    at = (p, pl.ds(y, 8), slice(None))
                    if i == 0:
                        out[at] = sol_ref[at] + alpha * step_ref[at]
                    else:
                        out[at] = res_ref[at] - alpha * moved_ref[at]
            planes = pl.ds(x, n)
            copies.append(pltpu.make_async_copy(out.at[planes], hbm.at[planes], sems.at[i, x // n]))
            copies[-1].start()
    for copy in copies:
        copy.wait()


def solution(mesh):
    px, py = mesh.shape["gx"], mesh.shape["gy"]

    def shards(right_side, guess, diagonal):
        LX, LY, LZ = guess.shape
        rows = 16
        NC, ZC = LY // rows, LZ // 128
        n = STEPS + 1
        dma = pltpu.SemaphoreType.DMA
        like = jax.ShapeDtypeStruct(guess.shape, jnp.float32)
        vmem, hbm = pl.BlockSpec(memory_space=pltpu.VMEM), pl.BlockSpec(memory_space=pltpu.MemorySpace.HBM)
        parts = pl.pallas_call(
            functools.partial(kernel, px, py, rows),
            out_shape=(like,) * 4 + (jax.ShapeDtypeStruct((8, 128), jnp.float32),),
            in_specs=[hbm] * 3,
            out_specs=(vmem,) * 5,
            scratch_shapes=[
                pltpu.VMEM((n + 1, ZC, LX + 2, LY + 3 * PAD, 128), jnp.float32),
                pltpu.VMEM((ZC, LX, LY, 128), jnp.float32),
                pltpu.VMEM((ZC, LX, LY, 128), jnp.float32),
                pltpu.VMEM((n, 2, ZC, LX, 128), jnp.float32),
                pltpu.VMEM((n, 2, ZC, LX, 128), jnp.float32),
                pltpu.VMEM((2, 1, 128), jnp.float32),
                pltpu.VMEM((2, px * py, 1, 128), jnp.float32),
                pltpu.VMEM((2 * STEPS + 1, 8, 128), jnp.float32),
                dma((ZC, 2)), dma((3, ZC)), dma((n, 2, NC)), dma((n, 2, NC)), dma((n, 2)), dma((n, 2)),
                dma((2,)), dma((2,)),
                pltpu.SemaphoreType.REGULAR((len(reach(px, 1)) + len(reach(py, 0)),)),
            ],
            compiler_params=pltpu.CompilerParams(
                collective_id=0, has_side_effects=True, vmem_limit_bytes=44 * 1024 * 1024
            ),
        )(right_side, guess, diagonal)
        return pl.pallas_call(
            last_step,
            out_shape=(like,) * 2,
            in_specs=[vmem] * 5,
            out_specs=(hbm,) * 2,
            scratch_shapes=[pltpu.VMEM(guess.shape, jnp.float32)] * 2 + [dma((2, LX))],
            compiler_params=pltpu.CompilerParams(vmem_limit_bytes=40 * 1024 * 1024),
        )(*parts)

    spec = P("gx", "gy", None)
    return jax.shard_map(
        shards, mesh=mesh, in_specs=(spec,) * 3, out_specs=(spec,) * 2, check_vma=False
    )
```

```python
import functools
import jax
import jax.numpy as jnp
from jax import lax
from jax.experimental import pallas as pl
from jax.experimental.pallas import tpu as pltpu
from jax.sharding import PartitionSpec as P

STEPS = 4
center_shift = 6.25
half_range = 6.25
PAD = 8
MESH = pl.DeviceIdType.MESH


def change_matrix(depth):
    rows = []
    for i in range(depth + 1):
        line = []
        for k in range(depth + 1):
            value = 0.0
            if k == 0:
                value = center_shift if i == 0 else half_range if i == 1 else 0.0
            elif k < depth:
                if i == k:
                    value = center_shift
                elif i == k - 1 or i == k + 1:
                    value = half_range / 2.0
            line.append(value)
        rows.append(line)
    return rows


def total(terms):
    terms = list(terms)
    while len(terms) > 1:
        pairs = [a + b for a, b in zip(terms[::2], terms[1::2])]
        terms = pairs + ([terms[-1]] if len(terms) % 2 else [])
    return terms[0]


def quad(left, gram, right):
    return total(l * total(g * r for g, r in zip(line, right)) for l, line in zip(left, gram))


def moved_by(change, pc):
    lines = [[c * p for c, p in zip(line, pc) if c != 0.0] for line in change]
    return [total(terms) for terms in lines]


def coefficient_steps(gram, depth, zero, one):
    change = [line[:depth] for line in change_matrix(depth)]
    unit = [one] + [zero] * (depth - 1)
    xc, rc, pc = [zero] * depth, unit, unit
    rr = quad(rc, gram, rc)
    for step in range(depth - 1):
        moved = moved_by(change[:depth], pc)
        alpha = rr / quad(pc, gram, moved)
        xc = [x + alpha * p for x, p in zip(xc, pc)]
        rc = [r - alpha * m for r, m in zip(rc, moved)]
        new = quad(rc, gram, rc)
        beta = new / rr
        pc = [r + beta * p for r, p in zip(rc, pc)]
        rr = new
    moved = moved_by(change, pc)
    return xc + [zero], rc + [zero], pc + [zero], moved, rr


def gram_of(moments, size):
    return [
        [0.5 * (moments[i + j] + moments[abs(i - j)]) for j in range(size)] for i in range(size)
    ]


def reach(count, known):
    steps = []
    while known < count - 1:
        steps.append(max(known, 1))
        known += steps[-1]
    return steps


def fold(p):
    rows, cols = p.shape
    return total(
        p[i : i + 8, j : j + 128] for i in range(0, rows, 8) for j in range(0, cols, 128)
    )


def kernel(px, py, rows, r_hbm, g_hbm, d_hbm, sol_out, step_out, res_out, moved_out, alpha_out,
           F, R, D, Ys, Yr, A, M, acc,
           edge_sem, load_sem, xs_sem, xr_sem, ys_sem, yr_sem, as_sem, ar_sem, met_sem):
    ZC, LX, LY, _ = R.shape
    NC = LY // rows
    gx, gy = lax.axis_index("gx"), lax.axis_index("gy")
    low_x, high_x, low_y, high_y = gx > 0, gx < px - 1, gy > 0, gy < py - 1
    inner = pl.ds(PAD, LY)

    def column(z):
        return pl.ds(z * 128, 128)

    edges, loads = [], []
    for z in range(ZC):
        for i, x in enumerate((0, LX - 1)):
            edges.append(pltpu.make_async_copy(
                g_hbm.at[x, :, column(z)], F.at[0, z, x + 1, inner, :], edge_sem.at[z, i]))
    for z in range(ZC):
        loads.append(pltpu.make_async_copy(
            g_hbm.at[pl.ds(1, LX - 2), :, column(z)],
            F.at[0, z, pl.ds(2, LX - 2), inner, :], load_sem.at[0, z]))
    for i, (src, dst) in enumerate(((d_hbm, D), (r_hbm, R))):
        for z in range(ZC):
            loads.append(pltpu.make_async_copy(
                src.at[:, :, column(z)], dst.at[z], load_sem.at[1 + i, z]))
    for copy in edges + loads:
        copy.start()

    x_has, y_has = (low_x, high_x), (low_y, high_y)

    def partners(axis, distance):
        me, count = (gx, px) if axis == "gx" else (gy, py)
        return [(me >= distance, {axis: me - distance}), (me < count - distance, {axis: me + distance})]

    def greet(sem, pairs):
        for there, device in pairs:
            pl.when(there)(lambda: pl.semaphore_signal(sem, inc=1, device_id=device, device_id_type=MESH))

    def meet(sem, pairs):
        pl.semaphore_wait(sem, sum(there.astype(jnp.int32) for there, _ in pairs))

    barrier = pltpu.get_barrier_semaphore()
    beside = partners("gx", 1) + partners("gy", 1)
    greet(barrier, beside)

    def zero_planes(x):
        def one(j, carry):
            at = pl.multiple_of(PAD + j * 8, 8)
            for k in range(STEPS + 1):
                for z in range(ZC):
                    F[k, z, x, pl.ds(at, 8), :] = jnp.zeros((8, 128), jnp.float32)
            return carry
        lax.fori_loop(0, LY // 8, one, 0)

    pl.when(jnp.logical_not(low_x))(lambda: zero_planes(0))
    pl.when(jnp.logical_not(high_x))(lambda: zero_planes(LX + 1))

    def zero_rows(side):
        for k in range(STEPS + 1):
            Yr[k, side] = jnp.zeros((ZC, LX, 128), jnp.float32)

    pl.when(jnp.logical_not(low_y))(lambda: zero_rows(0))
    pl.when(jnp.logical_not(high_y))(lambda: zero_rows(1))

    meet(barrier, beside)

    meetings = [("gx", o) for o in reach(px, 1)] + [("gy", o) for o in reach(py, 0)]
    met = []

    def spread(last=False):
        while len(met) <= len(meetings):
            n = len(met)
            if n > 0:
                meet(met_sem.at[n - 1], partners(*meetings[n - 1]))
            if n < len(meetings):
                greet(met_sem.at[n], partners(*meetings[n]))
            met.append(n)
            if not last:
                break

    me = gx * py + gy

    def send_sums(stage, row):
        A[stage] = row
        M[stage, me] = row
        for ox in range(px):
            to_x = jnp.where(gx < px // 2, px - 1 - ox, ox)
            for oy in range(py):
                to_y = jnp.where(gy < py // 2, py - 1 - oy, oy)

                @pl.when(jnp.logical_or(to_x != gx, to_y != gy))
                def _():
                    pltpu.make_async_remote_copy(
                        src_ref=A.at[stage], dst_ref=M.at[stage, me],
                        send_sem=as_sem.at[stage], recv_sem=ar_sem.at[stage],
                        device_id={"gx": to_x, "gy": to_y}, device_id_type=MESH,
                    ).start()

    def all_sums(stage):
        peers = pl.ds(0, px * py - 1)
        return pltpu.make_async_remote_copy(
            src_ref=M.at[stage, peers], dst_ref=M.at[stage, peers],
            send_sem=as_sem.at[stage], recv_sem=ar_sem.at[stage],
            device_id={"gx": lax.rem(gx + 1, px)}, device_id_type=MESH,
        )

    def x_copy(k, side, j):
        at = pl.ds(PAD + j * rows, rows)
        return pltpu.make_async_remote_copy(
            src_ref=F.at[k, :, 1 if side == 0 else LX, at, :],
            dst_ref=F.at[k, :, LX + 1 if side == 0 else 0, at, :],
            send_sem=xs_sem.at[k, side, j],
            recv_sem=xr_sem.at[k, side, j],
            device_id={"gx": gx - 1 if side == 0 else gx + 1},
            device_id_type=MESH,
        )

    def y_copy(k, side):
        return pltpu.make_async_remote_copy(
            src_ref=Ys.at[k, side],
            dst_ref=Yr.at[k, 1 - side],
            send_sem=ys_sem.at[k, side],
            recv_sem=yr_sem.at[k, side],
            device_id={"gy": gy - 1 if side == 0 else gy + 1},
            device_id_type=MESH,
        )

    def send_x(k, j, sides=(0, 1)):
        for side in sides:
            pl.when(x_has[side])(lambda: x_copy(k, side, j).start())

    def wait_x(k, j, sides=(0, 1)):
        for side in sides:
            pl.when(x_has[1 - side])(lambda: x_copy(k, side, j).wait_recv())

    def send_y(k):
        for x in range(LX):
            for z in range(ZC):
                Ys[k, 0, z, x : x + 1, :] = F[k, z, x + 1, PAD : PAD + 1, :]
                Ys[k, 1, z, x : x + 1, :] = F[k, z, x + 1, PAD + LY - 1 : PAD + LY, :]
        for side in (0, 1):
            pl.when(y_has[side])(lambda: y_copy(k, side).start())

    def wait_y(k):
        for side in (0, 1):
            pl.when(y_has[1 - side])(lambda: y_copy(k, side).wait_recv())
        for x in range(LX):
            for z in range(ZC):
                F[k, z, x + 1, PAD - 1 : PAD, :] = Yr[k, 0, z, x : x + 1, :]
                F[k, z, x + 1, PAD + LY : PAD + LY + 1, :] = Yr[k, 1, z, x : x + 1, :]

    order = [0] + ([NC - 1] if NC > 1 else []) + list(range(1, NC - 1))
    for copy in edges:
        copy.wait()
    for j in order:
        send_x(0, j)

    acc[...] = jnp.zeros(acc.shape, jnp.float32)
    zero_tile = jnp.zeros((8, 128), jnp.float32)

    c_scale = 2.0 / half_range

    def block(k, x, y, n, without=None):
        at, up, down = pl.ds(PAD + y, n), pl.ds(PAD + y + 1, n), pl.ds(PAD + y - 1, n)
        lane = lax.broadcasted_iota(jnp.int32, (n, 128), 1)
        first_lane, last_lane = lane == 0, lane == 127
        here = [F[k - 1, z, x, at, :] for z in range(ZC)]
        right = [pltpu.roll(h, 1, 1) for h in here]
        left = [pltpu.roll(h, 127, 1) for h in here]
        squares, crosses = [], []
        for z in range(ZC):
            inside = [p for p in (x + 1, x - 1) if without is None or p != without]
            beside = total(F[k - 1, z, p, at, :] for p in inside)
            beside = beside + (F[k - 1, z, x, up, :] + F[k - 1, z, x, down, :])
            before = jnp.where(first_lane, right[z - 1] if z > 0 else 0.0, right[z])
            after = jnp.where(last_lane, left[z + 1] if z < ZC - 1 else 0.0, left[z])
            beside = beside + (before + after)
            diag = D[z, x - 1, pl.ds(y, n), :]
            if k == 1:
                new = R[z, x - 1, pl.ds(y, n), :] - ((6.0 + diag) * here[z] - beside)
                D[z, x - 1, pl.ds(y, n), :] = (diag + (6.0 - center_shift)) * c_scale
            elif k == 2:
                new = (diag * here[z] - beside * c_scale) * 0.5
            else:
                new = diag * here[z] - beside * c_scale - F[k - 2, z, x, at, :]
            F[k, z, x, at, :] = new
            if without is not None:
                continue
            squares.append(fold(new * new))
            if k > 1:
                crosses.append(fold(new * here[z]))
        if without is None:
            return total(squares), (total(crosses) if k > 1 else zero_tile)

    def complete(k, x, beyond, y, n):
        at = pl.ds(PAD + y, n)
        squares, crosses = [], []
        for z in range(ZC):
            new = F[k, z, x, at, :] - c_scale * F[k - 1, z, beyond, at, :]
            F[k, z, x, at, :] = new
            squares.append(fold(new * new))
            crosses.append(fold(new * F[k - 1, z, x, at, :]))
        return total(squares), total(crosses)

    def add(a, b):
        return a[0] + b[0], a[1] + b[1]

    for copy in loads[:ZC]:
        copy.wait()
    send_y(0)
    for copy in loads[ZC:]:
        copy.wait()

    lane = lax.broadcasted_iota(jnp.int32, (1, 128), 1)

    def row_of(sums):
        row = jnp.zeros((1, 128), jnp.float32)
        for m, part in sums:
            s = jnp.sum(jnp.sum(part, axis=0, keepdims=True), axis=1, keepdims=True)
            row = row + jnp.where(lane == m, s, 0.0)
        return row

    def moments_of(stage, which):
        all_sums(stage).wait_recv()
        row = total(M[stage, i] for i in range(px * py))
        return {
            m: jnp.broadcast_to(jnp.sum(jnp.where(lane == m, row, 0.0), axis=1, keepdims=True), (8, 128))
            for m in which
        }

    for k in range(1, STEPS + 1):
        sums = (zero_tile, zero_tile)
        wait_y(k - 1)
        for i, j in enumerate(order):
            for side, x in ((0, 1), (1, LX)):
                wait_x(k - 1, j, (1 - side,))
                sums = add(sums, block(k, x, j * rows, rows))
                send_x(k, j, (side,))
            if i == 1:
                send_y(k)
            if i == 0:
                spans = [(0, 8), (LY - 8, 8)]
            elif i < NC - 1:
                spans = [(8 + (i - 1) * rows, rows)]
            else:
                spans = [(8 + (i - 1) * rows, LY - 16 - (i - 1) * rows)]

            def plane(x, s):
                for y, n in spans:
                    s = add(s, block(k, x, y, n))
                return s

            sums = lax.fori_loop(2, LX, plane, sums, unroll=7 if (LX - 2) % 7 == 0 else 2)
            if i % 2 == 0:
                spread()
        acc[2 * (k - 1)] = sums[0]
        if k > 1:
            acc[2 * (k - 1) - 1] = sums[1]

    spread(last=True)
    early, late = range(2 * STEPS - 1), range(2 * STEPS - 1, 2 * STEPS + 1)
    send_sums(0, row_of([(m, acc[m]) for m in early]))

    last = STEPS + 1
    wait_y(last - 1)

    def inner_plane(x, s):
        for y in range(0, LY, rows):
            s = add(s, block(last, x, y, rows))
        return s

    sums = lax.fori_loop(2, LX, inner_plane, (zero_tile, zero_tile))
    ends = ((1, 0), (LX, LX + 1))
    for x, beyond in ends:
        for j in order:
            block(last, x, j * rows, rows, without=beyond)
    for j in order:
        for side, (x, beyond) in enumerate(ends):
            wait_x(last - 1, j, (1 - side,))
            sums = add(sums, complete(last, x, beyond, j * rows, rows))
    send_sums(1, row_of([(2 * STEPS - 1, sums[1]), (2 * STEPS, sums[0])]))

    got = moments_of(0, early)

    def moment(m):
        return got[m] if m < 2 else 2.0 * got[m] - got[m % 2]

    moments = [moment(m) for m in early]
    zero, one = jnp.zeros((8, 128), jnp.float32), jnp.ones((8, 128), jnp.float32)
    xc, rc, pc, moved, rr = coefficient_steps(gram_of(moments, STEPS), STEPS, zero, one)

    def plane(x, carry):
        for i in range(LY // 8):
            at, to = pl.ds(PAD + i * 8, 8), pl.ds(i * 8, 8)
            for z in range(ZC):
                basis = [F[k + 1, z, x + 1, at, :] for k in range(STEPS + 1)]
                sol = F[0, z, x + 1, at, :]
                for k in range(STEPS + 1):
                    sol = sol + xc[k] * basis[k]
                sol_out[x, to, column(z)] = sol
                for out, coefficients in ((step_out, pc), (res_out, rc), (moved_out, moved)):
                    out[x, to, column(z)] = total(c * b for c, b in zip(coefficients, basis))
        return carry

    lax.fori_loop(0, LX, plane, 0)

    for k in range(STEPS + 1):
        for side in (0, 1):
            def done():
                for j in range(NC):
                    x_copy(k, side, j).wait_send()
            pl.when(x_has[side])(done)
            pl.when(y_has[side])(lambda: y_copy(k, side).wait_send())
    all_sums(0).wait_send()

    got.update(moments_of(1, late))
    moments += [moment(m) for m in late]
    alpha_out[...] = rr / quad(pc, gram_of(moments, STEPS + 1), moved)

    all_sums(1).wait_send()


def last_step(sol_ref, step_ref, res_ref, moved_ref, alpha_ref, sol_hbm, res_hbm, sol, res, sems):
    LX, LY, LZ = sol.shape
    alpha = jnp.concatenate([alpha_ref[...]] * (LZ // 128), axis=1)
    n = 1
    copies = []
    for x in range(0, LX, n):
        for i, (out, hbm) in enumerate(((sol, sol_hbm), (res, res_hbm))):
            for p in range(x, x + n):
                for y in range(0, LY, 8):
                    at = (p, pl.ds(y, 8), slice(None))
                    if i == 0:
                        out[at] = sol_ref[at] + alpha * step_ref[at]
                    else:
                        out[at] = res_ref[at] - alpha * moved_ref[at]
            planes = pl.ds(x, n)
            copies.append(pltpu.make_async_copy(out.at[planes], hbm.at[planes], sems.at[i, x // n]))
            copies[-1].start()
    for copy in copies:
        copy.wait()


def solution(mesh):
    px, py = mesh.shape["gx"], mesh.shape["gy"]

    def shards(right_side, guess, diagonal):
        LX, LY, LZ = guess.shape
        rows = 16
        NC, ZC = LY // rows, LZ // 128
        n = STEPS + 1
        dma = pltpu.SemaphoreType.DMA
        like = jax.ShapeDtypeStruct(guess.shape, jnp.float32)
        vmem, hbm = pl.BlockSpec(memory_space=pltpu.VMEM), pl.BlockSpec(memory_space=pltpu.MemorySpace.HBM)
        parts = pl.pallas_call(
            functools.partial(kernel, px, py, rows),
            out_shape=(like,) * 4 + (jax.ShapeDtypeStruct((8, 128), jnp.float32),),
            in_specs=[hbm] * 3,
            out_specs=(vmem,) * 5,
            scratch_shapes=[
                pltpu.VMEM((n + 1, ZC, LX + 2, LY + 3 * PAD, 128), jnp.float32),
                pltpu.VMEM((ZC, LX, LY, 128), jnp.float32),
                pltpu.VMEM((ZC, LX, LY, 128), jnp.float32),
                pltpu.VMEM((n, 2, ZC, LX, 128), jnp.float32),
                pltpu.VMEM((n, 2, ZC, LX, 128), jnp.float32),
                pltpu.VMEM((2, 1, 128), jnp.float32),
                pltpu.VMEM((2, px * py, 1, 128), jnp.float32),
                pltpu.VMEM((2 * STEPS + 1, 8, 128), jnp.float32),
                dma((ZC, 2)), dma((3, ZC)), dma((n, 2, NC)), dma((n, 2, NC)), dma((n, 2)), dma((n, 2)),
                dma((2,)), dma((2,)),
                pltpu.SemaphoreType.REGULAR((len(reach(px, 1)) + len(reach(py, 0)),)),
            ],
            compiler_params=pltpu.CompilerParams(
                collective_id=0, has_side_effects=True, vmem_limit_bytes=44 * 1024 * 1024
            ),
        )(right_side, guess, diagonal)
        return pl.pallas_call(
            last_step,
            out_shape=(like,) * 2,
            in_specs=[vmem] * 5,
            out_specs=(hbm,) * 2,
            scratch_shapes=[pltpu.VMEM(guess.shape, jnp.float32)] * 2 + [dma((2, LX))],
            compiler_params=pltpu.CompilerParams(vmem_limit_bytes=40 * 1024 * 1024),
        )(*parts)

    spec = P("gx", "gy", None)
    return jax.shard_map(
        shards, mesh=mesh, in_specs=(spec,) * 3, out_specs=(spec,) * 2, check_vma=False
    )
```
